64 devices in a mesh: dp: 4 (over x, y), ep: 16 (over z, core).
Axes of the slice: x: 2, y: 2, z: 8, core: 2. Of those that a mesh axis runs over, the one named last changes fastest.
The devices are a block of a 4x4x8 slice.
Arguments:
- x_in: bfloat16 [1536, 2048], P(('dp', 'ep')), parts along dimension 0
- topk_idx: int32 [1536, 8], P(('dp', 'ep')), parts along dimension 0
- topk_w: float32 [1536, 8], P(('dp', 'ep')), parts along dimension 0
- w_up: bfloat16 [64, 2048, 1024], P('ep')
- w_down: bfloat16 [64, 1024, 2048], P('ep')
Outputs:
- output: bfloat16 [1536, 2048], P(('dp', 'ep')), parts along dimension 0
There are 4 independent parts. The reference program is written for one: setup_inputs(seed, part) draws one part's arguments, and reference() takes and returns one part's arrays. A program takes and returns all parts, laid end to end along the dimension named above; an argument that names none is the same for every part.
All inputs are finite; a program needn't handle non-finite values.
Results may differ from the reference program's by a relative error of at most 0.001.
Values are sent between devices in bfloat16 or wider.
A program may use at most 768 MiB of HBM per device.

```python
import jax
import jax.numpy as jnp
from jax import lax

TOK_DEV = 24
GROUP_SIZE = 16
D_MODEL = 2048
D_FF = 1024
EXPERTS = 64
TOP_K = 8
TOKENS = TOK_DEV * GROUP_SIZE
PAIRS = TOKENS * TOP_K
ROW_WINDOW = min(64, TOKENS)


def draw_routing(route_key):
    key_perm, key_rank, key_start, key_roll = jax.random.split(route_key, 4)
    expert_order = jax.random.permutation(key_perm, EXPERTS).astype(jnp.int32)
    hot_pair = expert_order[:2]
    cold_cycle = expert_order[2:]
    cold_count = EXPERTS - 2
    ranks = jax.vmap(lambda one_key: jax.random.permutation(one_key, TOK_DEV))(jax.random.split(key_rank, GROUP_SIZE)).astype(jnp.int32)
    device_index = jnp.arange(GROUP_SIZE, dtype=jnp.int32)[:, None]
    cold_start = jax.random.randint(key_start, (), 0, cold_count, dtype=jnp.int32)
    cold_base = cold_start + (device_index * TOK_DEV + ranks) * (TOP_K - 1)
    cold_steps = jnp.arange(TOP_K - 1, dtype=jnp.int32)
    cold_ids = cold_cycle[(cold_base[:, :, None] + cold_steps) % cold_count]
    hot_ids = hot_pair[ranks % 2]
    picks = jnp.concatenate([hot_ids[:, :, None], cold_ids], axis=2).reshape(TOKENS, TOP_K)
    shifts = jax.random.randint(key_roll, (TOKENS, 1), 0, TOP_K, dtype=jnp.int32)
    slot_order = (jnp.arange(TOP_K, dtype=jnp.int32)[None, :] + shifts) % TOP_K
    return jnp.take_along_axis(picks, slot_order, axis=1)


def setup_inputs(seed: int = 0, part: int = 0) -> dict:
    part_key = jax.random.fold_in(jax.random.key(seed), part)
    key_x, key_route, key_gate = jax.random.split(part_key, 3)
    key_up, key_down = jax.random.split(jax.random.key(seed + 7919), 2)
    x_in = jax.random.normal(key_x, (TOKENS, D_MODEL), jnp.float32).astype(jnp.bfloat16)
    topk_idx = draw_routing(key_route)
    topk_w = jax.random.uniform(key_gate, (TOKENS, TOP_K), jnp.float32, 0.2, 1.0)
    w_up = lax.map(lambda one_key: (jax.random.normal(one_key, (D_MODEL, D_FF), jnp.float32) * D_MODEL ** -0.5).astype(jnp.bfloat16), jax.random.split(key_up, EXPERTS))
    w_down = lax.map(lambda one_key: (jax.random.normal(one_key, (D_FF, D_MODEL), jnp.float32) * D_FF ** -0.5).astype(jnp.bfloat16), jax.random.split(key_down, EXPERTS))
    return {'x_in': x_in, 'topk_idx': topk_idx, 'topk_w': topk_w, 'w_up': w_up, 'w_down': w_down}


def reference(x_in, topk_idx, topk_w, w_up, w_down):
    flat_ids = topk_idx.reshape(PAIRS)
    order = jnp.argsort(flat_ids, stable=True)
    pad_rows = jnp.zeros((ROW_WINDOW, D_MODEL), x_in.dtype)
    sorted_rows = jnp.concatenate([x_in[order // TOP_K], pad_rows], axis=0)
    counts = jnp.bincount(flat_ids, length=EXPERTS)
    starts = jnp.cumsum(counts) - counts

    def expert_step(expert, results):
        up_mat = w_up[expert]
        down_mat = w_down[expert]

        def window_step(window, acc_rows):
            base = starts[expert] + window * ROW_WINDOW
            rows = lax.dynamic_slice(sorted_rows, (base, 0), (ROW_WINDOW, D_MODEL))
            hidden = jax.nn.gelu(jnp.dot(rows, up_mat, preferred_element_type=jnp.float32), approximate=True).astype(jnp.bfloat16)
            result = jnp.dot(hidden, down_mat, preferred_element_type=jnp.float32).astype(jnp.bfloat16)
            valid = window * ROW_WINDOW + jnp.arange(ROW_WINDOW) < counts[expert]
            current = lax.dynamic_slice(acc_rows, (base, 0), (ROW_WINDOW, D_MODEL))
            return lax.dynamic_update_slice(acc_rows, jnp.where(valid[:, None], result, current), (base, 0))

        windows = (counts[expert] + ROW_WINDOW - 1) // ROW_WINDOW
        return lax.fori_loop(0, windows, window_step, results)

    results = jnp.zeros((PAIRS + ROW_WINDOW, D_MODEL), x_in.dtype)
    results = lax.fori_loop(0, EXPERTS, expert_step, results)
    pair_out = results[jnp.argsort(order)].reshape(TOKENS, TOP_K, D_MODEL)
    mixed = jnp.sum(topk_w[:, :, None] * pair_out.astype(jnp.float32), axis=1)
    return mixed.astype(jnp.bfloat16)
```

```python
import functools

import jax
import jax.numpy as jnp
from jax import lax
from jax.experimental import pallas as pl
from jax.experimental.pallas import tpu as pltpu
from jax.sharding import PartitionSpec as P

MESH = pl.DeviceIdType.MESH
X_CHUNKS = 4
OUT_COLS = 256
UP_COLS = 512
LAG = 3
GATE_LANES = 128


def moe_kernel(group, x_ref, idx_ref, gate_ref, wu_hbm, wd_hbm, y_ref, xr, gr, xa, ga, wu, wd, hid, pb, pp, sb, rb,
               w_sem, ag_send, ag_recv, ex_send, ex_recv, rs_send, rs_recv):
    chips = group // 2
    half = chips // 2
    tok, dim = x_ref.shape
    experts, _, ff = wu.shape
    blocks = pb.shape[0]
    cols = pb.shape[-1]
    width = xr.shape[-1]
    chunks = xr.shape[0]
    rows = group * tok
    me = lax.axis_index('ep')
    chip, core = me // 2, me % 2

    def dev(c, k):
        return lax.rem(c + 2 * chips, chips) * 2 + k

    right, left, partner = dev(chip + 1, core), dev(chip - 1, core), dev(chip, 1 - core)

    def up_copy(e):
        return pltpu.make_async_copy(wu_hbm.at[e], wu.at[e], w_sem.at[0, e])

    def down_copy(e):
        return pltpu.make_async_copy(wd_hbm.at[e], wd.at[e], w_sem.at[1, e])

    for e in range(experts):
        up_copy(e).start()
    for e in range(experts):
        down_copy(e).start()

    barrier = pltpu.get_barrier_semaphore()
    for peer in (left, right, partner):
        pl.semaphore_signal(barrier, inc=1, device_id={'ep': peer}, device_id_type=MESH)

    lane = lax.broadcasted_iota(jnp.int32, (tok, GATE_LANES), 1)
    dense = jnp.zeros((tok, GATE_LANES), jnp.float32)
    for j in range(idx_ref.shape[1]):
        dense = dense + jnp.where(idx_ref[:, j:j + 1] == lane, gate_ref[:, j:j + 1], 0.0)
    gr[me] = dense
    for k in range(chunks):
        xr[k, me] = x_ref[:, k * width:(k + 1) * width]
    pl.semaphore_wait(barrier, 3)

    def slot(k, d):
        return gr.at[d] if k == chunks else xr.at[k, d]

    def source(k, d):
        if d is None:
            return gr.at[me] if k == chunks else x_ref.at[:, pl.ds(k * width, width)]
        return slot(k, d)

    def ag(k, d, peer, send):
        src = slot(k, me) if d is None else slot(k, d)
        owner = me if d is None else d
        return pltpu.make_async_remote_copy(
            src_ref=source(k, d), dst_ref=slot(k, owner), send_sem=ag_send.at[k, send], recv_sem=ag_recv.at[k, owner],
            device_id={'ep': peer}, device_id_type=MESH)

    sent = []

    def push(copy):
        copy.start()
        sent.append(copy)

    def far_right(k):
        return k % 2 == 0

    for k in range(chunks + 1):
        push(ag(k, None, right, 0))
        push(ag(k, None, left, half))
        push(ag(k, None, partner, 2 * half))
    for s in range(half):
        for k in range(chunks + 1):
            if s < half - 1 or far_right(k):
                d = dev(chip - 1 - s, core)
                ag(k, d, right, 0).wait_recv()
                if s + 1 < half - 1 or (s + 1 == half - 1 and far_right(k)):
                    push(ag(k, d, right, 1 + s))
                push(ag(k, d, partner, 2 * half + 1 + s))
            if s < half - 1 or not far_right(k):
                d = dev(chip + 1 + s, core)
                ag(k, d, left, half).wait_recv()
                if s + 1 < half - 1 or (s + 1 == half - 1 and not far_right(k)):
                    push(ag(k, d, left, half + 1 + s))
                push(ag(k, d, partner, 3 * half + 1 + s))
    for k in range(chunks + 1):
        def arrive(c, carry):
            ag(k, c * 2 + 1 - core, partner, 0).wait_recv()
            return carry
        lax.fori_loop(0, chips, arrive, 0)
    for k in range(chunks):
        def relayout(c, carry):
            pair = jnp.concatenate([xr[k, 2 * c], xr[k, 2 * c + 1]], axis=0)
            xa[pl.ds(pl.multiple_of(c * 2 * tok, 2 * tok), 2 * tok), k * width:(k + 1) * width] = pair
            return carry
        lax.fori_loop(0, chips, relayout, 0)

    up_blocks = ff // UP_COLS

    def up_step(i, carry):
        e, nb = i // up_blocks, i % up_blocks

        @pl.when(nb == 0)
        def _():
            up_copy(e).wait()
        span = pl.ds(pl.multiple_of(nb * UP_COLS, UP_COLS), UP_COLS)
        z = jnp.dot(xa[...], wu[e, :, span], preferred_element_type=jnp.float32)
        hid[e, :, span] = jax.nn.gelu(z, approximate=True).astype(jnp.bfloat16)
        return carry

    lax.fori_loop(0, experts * up_blocks, up_step, 0)

    all_lane = lax.broadcasted_iota(jnp.int32, (rows, GATE_LANES), 1)
    all_gates = gr[...].reshape(rows, GATE_LANES)
    for e in range(experts):
        one = jnp.sum(jnp.where(all_lane == me * experts + e, all_gates, 0.0), axis=1, keepdims=True)
        ga[e] = jnp.broadcast_to(one, (rows, GATE_LANES))
    for e in range(experts):
        down_copy(e).wait()

    def compute(b):
        span = pl.ds(pl.multiple_of(b * cols, cols), cols)
        total = None
        for e in range(experts):
            out = jnp.dot(hid[e], wd[e, :, span], preferred_element_type=jnp.float32)
            out = out.astype(jnp.bfloat16).astype(jnp.float32)
            gate = jnp.concatenate([ga[e]] * (cols // GATE_LANES), axis=1)
            term = jnp.where(gate > 0, gate * out, 0.0)
            total = term if total is None else total + term
        pb[b] = total.reshape(chips, 2, tok, cols)

    def exchange(b):
        return pltpu.make_async_remote_copy(
            src_ref=pb.at[b, :, 1 - core], dst_ref=pp.at[b], send_sem=ex_send.at[b], recv_sem=ex_recv.at[b],
            device_id={'ep': partner}, device_id_type=MESH)

    def local(b, c):
        c = lax.rem(c + 2 * chips, chips)
        return pb[b, c, core] + pp[b, c]

    def message(b, m, sign):
        return pltpu.make_async_remote_copy(
            src_ref=sb.at[b, m], dst_ref=rb.at[b, m], send_sem=rs_send.at[b, m], recv_sem=rs_recv.at[b, m],
            device_id={'ep': dev(chip + sign, core)}, device_id_type=MESH)

    def hop(b, j):
        sign = 1 - 2 * (b % 2)
        if j < half:
            value = local(b, chip + sign * (half - j))
            if j > 0:
                message(b, j - 1, sign).wait_recv()
                value = value + rb[b, j - 1]
            sb[b, j] = value
            message(b, j, sign).start()
        if j + 1 < half:
            m = half + j
            value = local(b, chip - sign * (half - j - 1))
            if j > 0:
                message(b, m - 1, -sign).wait_recv()
                value = value + rb[b, m - 1]
            sb[b, m] = value
            message(b, m, -sign).start()

    def finish(b):
        sign = 1 - 2 * (b % 2)
        value = local(b, chip)
        message(b, 2 * half - 2, -sign).wait_recv()
        value = value + rb[b, 2 * half - 2]
        message(b, half - 1, sign).wait_recv()
        value = value + rb[b, half - 1]
        y_ref[:, pl.ds(pl.multiple_of(b * cols, cols), cols)] = value.astype(y_ref.dtype)

    def at(t, delay, work):
        b = t - delay

        @pl.when((b >= 0) & (b < blocks))
        def _():
            work(b)

    def round_step(t, carry):
        def first(b):
            compute(b)
            exchange(b).start()
        at(t, 0, first)

        def begin(b):
            exchange(b).wait_recv()
            hop(b, 0)
        at(t, 1, begin)
        for j in range(1, half):
            at(t, 1 + j * LAG, lambda b, j=j: hop(b, j))
        at(t, 1 + half * LAG, finish)
        return carry

    lax.fori_loop(0, blocks + 1 + half * LAG, round_step, 0)

    for copy in sent:
        copy.wait_send()

    def drain(b, carry):
        sign = 1 - 2 * (b % 2)
        exchange(b).wait_send()
        for m in range(2 * half - 1):
            message(b, m, sign).wait_send()
        return carry

    lax.fori_loop(0, blocks, drain, 0)


def solution(mesh):
    group = mesh.shape['ep']
    token_spec = P(('dp', 'ep'), None)
    expert_spec = P('ep', None, None)

    def local_layer(x_loc, ids_loc, gates_loc, w_up, w_down):
        tok, dim = x_loc.shape
        experts, _, ff = w_up.shape
        chips = group // 2
        half = chips // 2
        blocks = dim // OUT_COLS
        width = dim // X_CHUNKS
        rows = group * tok
        vmem = pl.BlockSpec(memory_space=pltpu.VMEM)
        hbm = pl.BlockSpec(memory_space=pl.ANY)
        msgs = 2 * half - 1
        return pl.pallas_call(
            functools.partial(moe_kernel, group),
            out_shape=jax.ShapeDtypeStruct((tok, dim), jnp.bfloat16),
            in_specs=[vmem, vmem, vmem, hbm, hbm],
            out_specs=vmem,
            scratch_shapes=[
                pltpu.VMEM((X_CHUNKS, group, tok, width), jnp.bfloat16),
                pltpu.VMEM((group, tok, GATE_LANES), jnp.float32),
                pltpu.VMEM((rows, dim), jnp.bfloat16),
                pltpu.VMEM((experts, rows, GATE_LANES), jnp.float32),
                pltpu.VMEM((experts, dim, ff), jnp.bfloat16),
                pltpu.VMEM((experts, ff, dim), jnp.bfloat16),
                pltpu.VMEM((experts, rows, ff), jnp.bfloat16),
                pltpu.VMEM((blocks, chips, 2, tok, OUT_COLS), jnp.float32),
                pltpu.VMEM((blocks, chips, tok, OUT_COLS), jnp.float32),
                pltpu.VMEM((blocks, msgs, tok, OUT_COLS), jnp.float32),
                pltpu.VMEM((blocks, msgs, tok, OUT_COLS), jnp.float32),
                pltpu.SemaphoreType.DMA((2, experts)),
                pltpu.SemaphoreType.DMA((X_CHUNKS + 1, 4 * half + 1)),
                pltpu.SemaphoreType.DMA((X_CHUNKS + 1, group)),
                pltpu.SemaphoreType.DMA((blocks,)),
                pltpu.SemaphoreType.DMA((blocks,)),
                pltpu.SemaphoreType.DMA((blocks, msgs)),
                pltpu.SemaphoreType.DMA((blocks, msgs)),
            ],
            compiler_params=pltpu.CompilerParams(collective_id=0, has_side_effects=True, vmem_limit_bytes=62 * 1024 * 1024),
        )(x_loc, ids_loc, gates_loc, w_up, w_down)

    return jax.shard_map(local_layer, mesh=mesh, in_specs=(token_spec, token_spec, token_spec, expert_spec, expert_spec), out_specs=token_spec, check_vma=False)
```
